32 devices in a mesh: gz: 2 (over x), gx: 4 (over y, core), gy: 4 (over z).
Axes of the slice: x: 2, y: 2, z: 4, core: 2. Of those that a mesh axis runs over, the one named last changes fastest.
Arguments:
- right_side: float32 [16, 3, 32, 1024], P('gz', None, 'gy', 'gx'), may hold values from -6 to 6
- start_field: float32 [16, 3, 32, 1024], P('gz', None, 'gy', 'gx'), may hold values from -6 to 6
- layer_material: int32 [16], P('gz'), may hold values from 0 to 7
- stiffness: float32 [8, 3, 3, 3], replicated, may hold values from -0.2 to 8, as said below
- line_factors: float32 [8, 3, 3, 3], replicated, may hold values from -0.05 to 1
Outputs:
- solution_field: float32 [16, 3, 32, 1024], P('gz', None, 'gy', 'gx')
- final_residual: float32 [16, 3, 32, 1024], P('gz', None, 'gy', 'gx')
The draws below stay inside these ranges and needn't reach their ends.
Inputs may be any that keep to these rules, and one draw needn't show every extreme that they name: `stiffness`: diagonal blocks dominate each row over the lateral and vertical couplings of the stencil.
All inputs are finite; a program needn't handle non-finite values.
Results may differ from the reference program's by a relative error of at most 0.0001.
Values sent between devices are 32-bit elements; how exact they have to be, the bound alone decides.
A program may use at most 64 MiB of HBM per device.

```python
import jax
import jax.numpy as jnp
from jax import lax

MATS = 8
SWEEPS = 3
NZ = 16
NY = 32
NX = 1024


def symmetric_noise(key, scale):
    noise = jax.random.uniform(key, (MATS, 3, 3), jnp.float32, -1.0, 1.0)
    both = 0.5 * (noise + jnp.swapaxes(noise, 1, 2))
    return scale * both * (1.0 - jnp.eye(3, dtype=jnp.float32))


def draw_stiffness(key, part):
    keys = jax.random.split(jax.random.fold_in(key, 11), 6)
    eye = jnp.eye(3, dtype=jnp.float32)
    lateral_rate = jax.random.uniform(keys[0], (MATS, 3), jnp.float32, 0.1, 0.3)
    vertical_rate = jax.random.uniform(keys[1], (MATS, 3), jnp.float32, 0.5, 1.5)
    margin = jax.random.uniform(keys[2], (MATS, 3), jnp.float32, 0.3, 1.0)
    lateral_off = symmetric_noise(keys[3], 0.03)
    vertical_off = symmetric_noise(keys[4], 0.1)
    diagonal_off = symmetric_noise(keys[5], 0.2)
    lateral_block = eye * lateral_rate[:, :, None] + lateral_off
    vertical_block = eye * vertical_rate[:, :, None] + vertical_off
    diagonal_value = 4.0 * lateral_rate + 2.0 * vertical_rate + margin
    diagonal_value = diagonal_value + 4.0 * jnp.sum(jnp.abs(lateral_off), axis=2)
    diagonal_value = diagonal_value + 2.0 * jnp.sum(jnp.abs(vertical_off), axis=2)
    diagonal_value = diagonal_value + jnp.sum(jnp.abs(diagonal_off), axis=2)
    diagonal_block = eye * diagonal_value[:, :, None] + diagonal_off
    return jnp.stack([diagonal_block, lateral_block, vertical_block], axis=1)


def draw_line_factors(key, part):
    keys = jax.random.split(jax.random.fold_in(key, 23), 8)
    eye = jnp.eye(3, dtype=jnp.float32)
    fast_comp = jax.random.randint(keys[0], (), 0, 3)
    quick_mask = jnp.arange(3)[None, :] == fast_comp

    def rates(first_key, second_key):
        slow = 1.0 - jnp.exp(jax.random.uniform(first_key, (MATS, 3), jnp.float32, jnp.log(1.0 / NZ), jnp.log(3.0 / NZ)))
        quick = 1.0 - jax.random.uniform(second_key, (MATS, 3), jnp.float32, 0.03, 0.08)
        return jnp.where(quick_mask, quick, slow)
    forward_rate = rates(keys[1], keys[2])
    backward_rate = rates(keys[3], keys[4])

    def multiplier(rate, sub_key):
        root = jnp.sqrt(1.0 - rate)
        coupling = 0.1 * root[:, :, None] * symmetric_noise(sub_key, 1.0) * root[:, None, :]
        return eye * rate[:, :, None] + coupling
    forward_block = multiplier(forward_rate, keys[5])
    backward_block = multiplier(backward_rate, keys[6])
    gain = 1.5 * (1.0 - forward_rate) * (1.0 - backward_rate)
    pivot_block = gain[:, :, None] * (eye + symmetric_noise(keys[7], 0.1))
    return jnp.stack([pivot_block, forward_block, backward_block], axis=1)


def touch_ends(values, stream_key, smallest, high):
    longest = values.shape.index(max(values.shape))
    spots = []
    for shift in (0, 1):
        where = [jax.random.randint(jax.random.fold_in(stream_key, axis), (), 0, length) for axis, length in enumerate(values.shape)]
        where[longest] = (where[longest] + shift) % values.shape[longest]
        spots.append(tuple(where))
    return values.at[spots[0]].set(smallest).at[spots[1]].set(high)


def levels(key, dims, shards, low, top_value):
    factor_of = 1.0
    for axis_at, parts in shards:
        steps = jax.random.uniform(jax.random.fold_in(jax.random.fold_in(key, 6), axis_at), (parts,), jnp.float32, low / len(shards), top_value / len(shards))
        factor_of = factor_of * jnp.repeat(jnp.exp(steps), dims[axis_at] // parts).reshape((-1,) + (1,) * (len(dims) - 1 - axis_at))
    return factor_of


def scatter_about(key, extent, spread, bound, cuts=(), kind=jnp.bfloat16):
    level = levels(key, extent, cuts, -0.22, 0.18) if cuts else 1.0
    drawn = jax.random.normal(key, extent, jnp.float32) * spread * level
    return jnp.minimum(jnp.maximum(drawn, -bound), bound).astype(kind)


def setup_inputs(seed: int = 0) -> dict:
    seeds = jax.random.split(jax.random.key(seed), 6)
    right_side = scatter_about(seeds[0], (NZ, 3, NY, NX), 1.0, 6.0, ((0, 2), (2, 4), (3, 4)), jnp.float32)
    start_field = scatter_about(seeds[1], (NZ, 3, NY, NX), 1.0, 6.0, ((0, 2), (2, 4), (3, 4)), jnp.float32)
    layer_material = touch_ends(jax.random.randint(seeds[2], (NZ,), 0, MATS), jax.random.fold_in(seeds[2], 1), 0, MATS - 1).astype(jnp.int32)
    stiffness = draw_stiffness(jax.random.fold_in(seeds[5], 71), 0)
    line_factors = draw_line_factors(jax.random.fold_in(seeds[5], 71), 0)
    return dict(right_side=right_side, start_field=start_field, layer_material=layer_material, stiffness=stiffness, line_factors=line_factors)


def apply_block(blocks, field):
    columns = []
    for row_index in range(3):
        summed = blocks[..., row_index, 0, None, None] * field[..., 0, :, :]
        for col_index in (1, 2):
            summed = summed + blocks[..., row_index, col_index, None, None] * field[..., col_index, :, :]
        columns.append(summed)
    return jnp.stack(columns, axis=-3)


def operate(field, diag_block, lateral_block, vertical_block):
    padded = jnp.pad(field, ((1, 1), (0, 0), (1, 1), (1, 1)))
    lateral = padded[1:-1, :, 1:-1, 2:] + padded[1:-1, :, 1:-1, :-2]
    lateral = lateral + padded[1:-1, :, 2:, 1:-1] + padded[1:-1, :, :-2, 1:-1]
    vertical = padded[2:, :, 1:-1, 1:-1] + padded[:-2, :, 1:-1, 1:-1]
    return apply_block(diag_block, field) - apply_block(lateral_block, lateral) - apply_block(vertical_block, vertical)


def line_solve(resid, factor_blocks):
    weighted = apply_block(factor_blocks[:, 0], resid)

    def advance(carry, item):
        multiplier, source = item
        nxt = source + apply_block(multiplier, carry)
        return nxt, nxt

    start = jnp.zeros(resid.shape[1:], jnp.float32)
    _, upward = lax.scan(advance, start, (factor_blocks[:, 1], weighted))
    _, downward = lax.scan(advance, start, (factor_blocks[:, 2], upward), reverse=True)
    return downward


def reference(right_side, start_field, layer_material, stiffness, line_factors):
    fine_sten = stiffness[layer_material]
    coarse_ids = layer_material[0::2]
    coarse_sten = stiffness[coarse_ids]
    fine_fac = line_factors[layer_material]
    coarse_fac = line_factors[coarse_ids]
    fine_args = (fine_sten[:, 0], fine_sten[:, 1], fine_sten[:, 2])
    coarse_args = (coarse_sten[:, 0], coarse_sten[:, 1], 0.25 * coarse_sten[:, 2])
    field = start_field
    for counter in range(SWEEPS):
        field = field + line_solve(right_side - operate(field, *fine_args), fine_fac)
    resid = right_side - operate(field, *fine_args)
    paired = resid.reshape(resid.shape[0] // 2, 2, 3, resid.shape[2], resid.shape[3])
    coarse_rhs = paired[:, 0] + paired[:, 1]
    correction = line_solve(coarse_rhs, coarse_fac)
    for counter in range(SWEEPS - 1):
        correction = correction + line_solve(coarse_rhs - operate(correction, *coarse_args), coarse_fac)
    solution_field = field + jnp.repeat(correction, 2, axis=0)
    final_residual = right_side - operate(solution_field, *fine_args)
    return solution_field, final_residual
```

```python
import functools

import jax
import jax.numpy as jnp
from jax import lax
from jax.experimental import pallas as pl
from jax.experimental.pallas import tpu as pltpu
from jax.sharding import PartitionSpec as P

SWEEPS = 3
MESH = pl.DeviceIdType.MESH


def total(terms):
    result = terms[0]
    for term in terms[1:]:
        result = result + term
    return result


def kernel(
    sizes, material, sten, fac, load, start, out_u, out_r,
    cor, crhs, res, loc, chain, below, above, cbelow, cabove,
    row_out, row_in, crow_out, crow_in, col_out, col_in,
    gather, maps,
    row_ss, row_rs, col_ss, col_rs, z_ss, z_rs, map_ss, map_rs, zh_ss, zh_rs,
):
    nz, ny, nx = sizes
    layers, comps, rows, lanes = load.shape
    half = layers // 2
    gz, gy, gx = (lax.axis_index(name) for name in ("gz", "gy", "gx"))
    wide = col_in.shape[-1]
    row_id = lax.broadcasted_iota(jnp.int32, (rows, lanes), 0)
    lane_id = lax.broadcasted_iota(jnp.int32, (rows, lanes), 1)
    col_id = lax.broadcasted_iota(jnp.int32, (rows, wide), 1)
    top, bottom = row_id == 0, row_id == rows - 1
    first, last = lane_id == 0, lane_id == lanes - 1
    three = range(comps)
    pending = []

    def block(table, level, layer, which):
        base = material[layer * (2 if level else 1)] * 27 + which * 9
        scale = 0.25 if level and table is sten and which == 2 else None
        values = [[table[base + i * 3 + j] for j in three] for i in three]
        if scale is not None:
            values = [[scale * v for v in line] for line in values]
        return values

    def times(mat, vec):
        return [total([mat[i][j] * vec[j] for j in three]) for i in three]

    def at(z, y, x):
        return {"gz": z, "gy": y, "gx": x}

    def copy_if(cond, src, dst, ss, rs, target):
        copy = pltpu.make_async_remote_copy(
            src_ref=src, dst_ref=dst, send_sem=ss, recv_sem=rs,
            device_id=target, device_id_type=MESH,
        )

        @pl.when(cond)
        def _():
            copy.start()

        pending.append((cond, copy))

    def arrive_if(cond, ref, ss, rs):
        @pl.when(cond)
        def _():
            pltpu.make_async_remote_copy(
                src_ref=ref, dst_ref=ref, send_sem=ss, recv_sem=rs,
                device_id=at(gz, gy, gx), device_id_type=MESH,
            ).wait_recv()

    has_prev_y, has_next_y = gy > 0, gy < ny - 1
    has_prev_x, has_next_x = gx > 0, gx < nx - 1
    has_below, has_above = gz > 0, gz < nz - 1

    barrier = pltpu.get_barrier_semaphore()
    peers = [(gz != j, at(j, gy, gx)) for j in range(nz)]
    peers += [(has_prev_y, at(gz, gy - 1, gx)), (has_next_y, at(gz, gy + 1, gx))]
    peers += [(has_prev_x, at(gz, gy, gx - 1)), (has_next_x, at(gz, gy, gx + 1))]
    for cond, target in peers:
        @pl.when(cond)
        def _(target=target):
            pl.semaphore_signal(barrier, inc=1, device_id=target, device_id_type=MESH)

    for side, cond in enumerate((has_prev_y, has_next_y)):
        @pl.when(jnp.logical_not(cond))
        def _(side=side):
            row_in[:, side] = jnp.zeros_like(row_in[:, side])
            crow_in[:, side] = jnp.zeros_like(crow_in[:, side])
    for side, cond in enumerate((has_prev_x, has_next_x)):
        @pl.when(jnp.logical_not(cond))
        def _(side=side):
            col_in[:, side] = jnp.zeros_like(col_in[:, side])
    for cond, ref in ((has_below, below), (has_above, above)):
        @pl.when(jnp.logical_not(cond))
        def _(ref=ref):
            ref[...] = jnp.zeros_like(ref)
    for j in range(nz):
        @pl.when(gz > j)
        def _(j=j):
            gather[:, 1, j] = jnp.zeros_like(gather[:, 1, j])

    basis_lane = lax.broadcasted_iota(jnp.int32, (8, 128), 1)
    basis = [(basis_lane == c).astype(jnp.float32) for c in three]
    for level, count in ((0, layers), (1, half)):
        ups = []
        carry = basis
        for layer in range(count):
            carry = times(block(fac, level, layer, 1), carry)
            ups.append(carry)
        turned, back = None, basis
        for layer in reversed(range(count)):
            mat = block(fac, level, layer, 2)
            turned = ups[layer] if turned is None else [
                a + b for a, b in zip(ups[layer], times(mat, turned))
            ]
            back = times(mat, back)
            if layer == count - 1:
                edge = back
        for kind, value in enumerate((ups[-1], turned, back, edge)):
            for c in three:
                maps[gz, level, kind, c] = value[c]

    def held(level, owner, kind):
        tiles = [maps[owner, level, kind, c] for c in three]
        return [[jnp.broadcast_to(tiles[i][:rows, j : j + 1], (rows, lanes)) for j in three] for i in three]

    def send_sides(phase, level, field, count):
        out, into = (crow_out, crow_in) if level else (row_out, row_in)
        slot = phase - SWEEPS - 1 if level else (phase if phase <= SWEEPS else SWEEPS + 1)
        tiles = [jnp.zeros((rows, wide), jnp.float32)] * 2
        for layer in range(count):
            for c in three:
                spot = layer * comps + c
                value = field[layer, c]
                out[slot, 0, spot : spot + 1, :] = value[rows - 1 : rows, :]
                out[slot, 1, spot : spot + 1, :] = value[0:1, :]
                here = col_id == spot
                tiles[0] = jnp.where(here, value[:, lanes - 1 : lanes], tiles[0])
                tiles[1] = jnp.where(here, value[:, 0:1], tiles[1])
        for side in range(2):
            col_out[phase, side] = tiles[side]
        for side, cond, target in (
            (0, has_next_y, at(gz, gy + 1, gx)), (1, has_prev_y, at(gz, gy - 1, gx)),
        ):
            copy_if(cond, out.at[slot, side], into.at[slot, side],
                    row_ss.at[phase, side], row_rs.at[phase, side], target)
        for side, cond, target in (
            (0, has_next_x, at(gz, gy, gx + 1)), (1, has_prev_x, at(gz, gy, gx - 1)),
        ):
            copy_if(cond, col_out.at[phase, side], col_in.at[phase, side],
                    col_ss.at[phase, side], col_rs.at[phase, side], target)
        return phase, slot, into

    def await_sides(handle):
        phase, slot, into = handle
        for side, cond in enumerate((has_prev_y, has_next_y)):
            arrive_if(cond, into.at[slot, side], row_ss.at[phase, side], row_rs.at[phase, side])
        for side, cond in enumerate((has_prev_x, has_next_x)):
            arrive_if(cond, col_in.at[phase, side], col_ss.at[phase, side], col_rs.at[phase, side])

    def inner_residual(level, field, source, low, high, count):
        for layer in range(count):
            here = [field[layer, c] for c in three]
            side, vert = [], []
            for c in three:
                x = here[c]
                side.append(
                    (jnp.where(first, 0.0, pltpu.roll(x, 1, 1)) + jnp.where(last, 0.0, pltpu.roll(x, lanes - 1, 1)))
                    + (jnp.where(top, 0.0, pltpu.roll(x, 1, 0)) + jnp.where(bottom, 0.0, pltpu.roll(x, rows - 1, 0)))
                )
                under = field[layer - 1, c] if layer else low[c]
                over = field[layer + 1, c] if layer < count - 1 else high[c]
                vert.append(under + over)
            a = times(block(sten, level, layer, 0), here)
            b = times(block(sten, level, layer, 1), side)
            d = times(block(sten, level, layer, 2), vert)
            for c in three:
                res[layer, c] = source[layer, c] - (a[c] - b[c] - d[c])

    def full_residual(level, handle, layer):
        phase, slot, into = handle
        edge = []
        for c in three:
            spot = layer * comps + c
            line = jnp.where(top, into[slot, 0, spot : spot + 1, :], 0.0)
            line = jnp.where(bottom, into[slot, 1, spot : spot + 1, :], line)
            post = jnp.where(first, col_in[phase, 0][:, spot : spot + 1], 0.0)
            post = jnp.where(last, col_in[phase, 1][:, spot : spot + 1], post)
            edge.append(line + post)
        extra = times(block(sten, level, layer, 1), edge)
        return [res[layer, c] + extra[c] for c in three]

    def line_solve(level, turn, resid, count):
        carry = None
        for layer in range(count):
            now = times(block(fac, level, layer, 0), resid(layer))
            if carry is not None:
                now = [a + b for a, b in zip(now, times(block(fac, level, layer, 1), carry))]
            for c in three:
                chain[layer, c] = now[c]
            carry = now
        for c in three:
            gather[turn, 0, gz, c] = carry[c]
        if nz > 1:
            for j in range(nz):
                copy_if(jnp.logical_and(gz != j, gz < nz - 1), gather.at[turn, 0, gz], gather.at[turn, 0, gz],
                        z_ss.at[turn, 0, j], z_rs.at[turn, 0, gz], at(j, gy, gx))
        back = None
        for layer in reversed(range(count)):
            now = [chain[layer, c] for c in three]
            if back is not None:
                now = [a + b for a, b in zip(now, times(block(fac, level, layer, 2), back))]
            for c in three:
                loc[layer, c] = now[c]
            back = now
        for c in three:
            gather[turn, 1, gz, c] = back[c]
        for j in range(nz):
            copy_if(gz > j, gather.at[turn, 1, gz], gather.at[turn, 1, gz],
                    z_ss.at[turn, 1, j], z_rs.at[turn, 1, gz], at(j, gy, gx))
        for j in range(nz - 1):
            arrive_if(gz != j, gather.at[turn, 0, j], z_ss.at[turn, 0, j], z_rs.at[turn, 0, j])
        for j in range(1, nz):
            arrive_if(gz < j, gather.at[turn, 1, j], z_ss.at[turn, 1, j], z_rs.at[turn, 1, j])
        zero = [jnp.zeros((rows, lanes), jnp.float32)] * 3
        ins, outs = [zero], [zero]
        for k in range(nz - 1):
            value = [gather[turn, 0, k, c] for c in three]
            if k:
                value = [a + b for a, b in zip(value, times(held(level, k, 0), ins[k]))]
            ins.append(value)
        for k in reversed(range(1, nz)):
            value = [gather[turn, 1, k, c] + b for c, b in enumerate(times(held(level, k, 1), ins[k]))]
            if k < nz - 1:
                value = [a + b for a, b in zip(value, times(held(level, k, 2), outs[0]))]
            outs.insert(0, value)
        enter, leave = ins[0], outs[0]
        for k in range(1, nz):
            enter = [jnp.where(gz == k, a, b) for a, b in zip(ins[k], enter)]
            leave = [jnp.where(gz == k, a, b) for a, b in zip(outs[k], leave)]
        carry = enter
        for layer in range(count):
            carry = times(block(fac, level, layer, 1), carry)
            for c in three:
                chain[layer, c] = carry[c]
        carry = leave
        for layer in reversed(range(count)):
            carry = [chain[layer, c] + b for c, b in enumerate(times(block(fac, level, layer, 2), carry))]
            for c in three:
                loc[layer, c] = loc[layer, c] + carry[c]
        under = times(held(level, jnp.maximum(gz - 1, 0), 3), [loc[0, c] for c in three])
        under = [jnp.where(has_below, enter[c] + under[c], 0.0) for c in three]
        return under, leave

    pl.semaphore_wait(barrier, total([cond.astype(jnp.int32) for cond, _ in peers]))

    handle = send_sides(0, 0, start, layers)
    copy_if(has_above, start.at[layers - 1], below, zh_ss.at[0], zh_rs.at[0], at(gz + 1, gy, gx))
    copy_if(has_below, start.at[0], above, zh_ss.at[1], zh_rs.at[1], at(gz - 1, gy, gx))
    for j in range(nz):
        copy_if(gz != j, maps.at[gz], maps.at[gz], map_ss.at[j], map_rs.at[gz], at(j, gy, gx))
    arrive_if(has_below, below, zh_ss.at[0], zh_rs.at[0])
    arrive_if(has_above, above, zh_ss.at[1], zh_rs.at[1])
    for sweep in range(SWEEPS + 1):
        field = out_u if sweep else start
        inner_residual(0, field, load, below, above, layers)
        await_sides(handle)
        if sweep == SWEEPS:
            break
        if sweep == 0:
            for j in range(nz):
                arrive_if(gz != j, maps.at[j], map_ss.at[j], map_rs.at[j])
        under, over = line_solve(0, sweep, functools.partial(full_residual, 0, handle), layers)
        for layer in range(layers):
            for c in three:
                out_u[layer, c] = field[layer, c] + loc[layer, c]
        for c in three:
            below[c] = below[c] + under[c]
            above[c] = above[c] + over[c]
        handle = send_sides(sweep + 1, 0, out_u, layers)

    for k in range(half):
        pair = [full_residual(0, handle, 2 * k + step) for step in range(2)]
        for c in three:
            crhs[k, c] = pair[0][c] + pair[1][c]
    for sweep in range(SWEEPS):
        if sweep:
            inner_residual(1, cor, crhs, cbelow, cabove, half)
            await_sides(handle)
            source = functools.partial(full_residual, 1, handle)
        else:
            def source(layer):
                return [crhs[layer, c] for c in three]
        under, over = line_solve(1, SWEEPS + sweep, source, half)
        for layer in range(half):
            for c in three:
                value = loc[layer, c]
                cor[layer, c] = cor[layer, c] + value if sweep else value
        for c in three:
            cbelow[c] = cbelow[c] + under[c] if sweep else under[c]
            cabove[c] = cabove[c] + over[c] if sweep else over[c]
        if sweep < SWEEPS - 1:
            handle = send_sides(SWEEPS + 1 + sweep, 1, cor, half)
    for layer in range(layers):
        for c in three:
            out_u[layer, c] = out_u[layer, c] + cor[layer // 2, c]
    for c in three:
        below[c] = below[c] + cbelow[c]
        above[c] = above[c] + cabove[c]
    handle = send_sides(2 * SWEEPS, 0, out_u, layers)
    inner_residual(0, out_u, load, below, above, layers)
    await_sides(handle)
    for layer in range(layers):
        value = full_residual(0, handle, layer)
        for c in three:
            out_r[layer, c] = value[c]
    for cond, copy in pending:
        @pl.when(cond)
        def _(copy=copy):
            copy.wait_send()


def solution(mesh):
    sizes = tuple(mesh.shape[name] for name in ("gz", "gy", "gx"))
    nz = sizes[0]

    def on_device(right_side, start_field, layer_material, stiffness, line_factors):
        layers, comps, rows, lanes = right_side.shape
        half = layers // 2
        wide = -(-layers * comps // 128) * 128
        phases = 2 * SWEEPS + 1
        f32 = jnp.float32
        vmem = pl.BlockSpec(memory_space=pltpu.VMEM)
        smem = pl.BlockSpec(memory_space=pltpu.SMEM)
        dma = pltpu.SemaphoreType.DMA
        scratch = [
            pltpu.VMEM((half, comps, rows, lanes), f32),
            pltpu.VMEM((half, comps, rows, lanes), f32),
            pltpu.VMEM((layers, comps, rows, lanes), f32),
            pltpu.VMEM((layers, comps, rows, lanes), f32),
            pltpu.VMEM((layers, comps, rows, lanes), f32),
        ]
        scratch += [pltpu.VMEM((comps, rows, lanes), f32)] * 4
        scratch += [pltpu.VMEM((SWEEPS + 2, 2, layers * comps, lanes), f32)] * 2
        scratch += [pltpu.VMEM((SWEEPS - 1, 2, half * comps, lanes), f32)] * 2
        scratch += [pltpu.VMEM((phases, 2, rows, wide), f32)] * 2
        scratch += [
            pltpu.VMEM((2 * SWEEPS, 2, nz, comps, rows, lanes), f32),
            pltpu.VMEM((nz, 2, 4, comps, 8, 128), f32),
        ]
        scratch += [dma((phases, 2))] * 4 + [dma((2 * SWEEPS, 2, nz))] * 2
        scratch += [dma((nz,))] * 2 + [dma((2,))] * 2
        out = jax.ShapeDtypeStruct(right_side.shape, f32)
        return pl.pallas_call(
            functools.partial(kernel, sizes),
            out_shape=(out, out),
            in_specs=[smem, smem, smem, vmem, vmem],
            out_specs=(vmem, vmem),
            scratch_shapes=scratch,
            compiler_params=pltpu.CompilerParams(collective_id=0, has_side_effects=True),
        )(layer_material, stiffness.reshape(-1), line_factors.reshape(-1), right_side, start_field)

    return jax.shard_map(
        on_device,
        mesh=mesh,
        in_specs=(P("gz", None, "gy", "gx"), P("gz", None, "gy", "gx"), P("gz"), P(), P()),
        out_specs=(P("gz", None, "gy", "gx"), P("gz", None, "gy", "gx")),
        check_vma=False,
    )
```

```python
import functools

import jax
import jax.numpy as jnp
from jax import lax
from jax.experimental import pallas as pl
from jax.experimental.pallas import tpu as pltpu
from jax.sharding import PartitionSpec as P

SWEEPS = 3
MESH = pl.DeviceIdType.MESH


def total(terms):
    result = terms[0]
    for term in terms[1:]:
        result = result + term
    return result


def kernel(
    sizes, material, sten, fac, load, start, out_u, out_r,
    cor, crhs, res, loc, chain, chainx, hal, chal, below, above, cbelow, cabove,
    row_out, row_in, crow_out, crow_in, col_out, col_in,
    gather, maps, grow_out, grow_in, gcol_out, gcol_in,
    row_ss, row_rs, col_ss, col_rs, z_ss, z_rs, map_ss, map_rs, zh_ss, zh_rs,
    gr_ss, gr_rs, gc_ss, gc_rs,
):
    nz, ny, nx = sizes
    layers, comps, rows, lanes = load.shape
    half = layers // 2
    gz, gy, gx = (lax.axis_index(name) for name in ("gz", "gy", "gx"))
    wide = col_in.shape[-1]
    row_id = lax.broadcasted_iota(jnp.int32, (rows, lanes), 0)
    lane_id = lax.broadcasted_iota(jnp.int32, (rows, lanes), 1)
    col_id = lax.broadcasted_iota(jnp.int32, (rows, wide), 1)
    top, bottom = row_id == 0, row_id == rows - 1
    first, last = lane_id == 0, lane_id == lanes - 1
    three = range(comps)
    pending = []

    def block(table, level, layer, which):
        mat_id = material[layer * (2 if level else 1)]
        scale = 0.25 if level and table is sten and which == 2 else None
        values = [[table[which, i, j, mat_id] for j in three] for i in three]
        if scale is not None:
            values = [[scale * v for v in line] for line in values]
        return values

    def times(mat, vec):
        return [total([mat[i][j] * vec[j] for j in three]) for i in three]

    def at(z, y, x):
        return {"gz": z, "gy": y, "gx": x}

    def copy_if(cond, src, dst, ss, rs, target):
        copy = pltpu.make_async_remote_copy(
            src_ref=src, dst_ref=dst, send_sem=ss, recv_sem=rs,
            device_id=target, device_id_type=MESH,
        )

        @pl.when(cond)
        def _():
            copy.start()

        pending.append((cond, copy))

    def arrive_if(cond, ref, ss, rs):
        @pl.when(cond)
        def _():
            pltpu.make_async_remote_copy(
                src_ref=ref, dst_ref=ref, send_sem=ss, recv_sem=rs,
                device_id=at(gz, gy, gx), device_id_type=MESH,
            ).wait_recv()

    has_prev_y, has_next_y = gy > 0, gy < ny - 1
    has_prev_x, has_next_x = gx > 0, gx < nx - 1
    has_below, has_above = gz > 0, gz < nz - 1

    barrier = pltpu.get_barrier_semaphore()
    peers = [(gz != j, at(j, gy, gx)) for j in range(nz)]
    peers += [(has_prev_y, at(gz, gy - 1, gx)), (has_next_y, at(gz, gy + 1, gx))]
    peers += [(has_prev_x, at(gz, gy, gx - 1)), (has_next_x, at(gz, gy, gx + 1))]
    sides_y = ((has_next_y, gy + 1), (has_prev_y, gy - 1))
    sides_x = ((has_next_x, gx + 1), (has_prev_x, gx - 1))
    for j in range(nz):
        peers += [(jnp.logical_and(gz != j, cond), at(j, spot, gx)) for cond, spot in sides_y]
        peers += [(jnp.logical_and(gz != j, cond), at(j, gy, spot)) for cond, spot in sides_x]
    for cond, target in peers:
        @pl.when(cond)
        def _(target=target):
            pl.semaphore_signal(barrier, inc=1, device_id=target, device_id_type=MESH)

    for side, cond in enumerate((has_prev_y, has_next_y)):
        @pl.when(jnp.logical_not(cond))
        def _(side=side):
            row_in[:, side] = jnp.zeros_like(row_in[:, side])
            crow_in[:, side] = jnp.zeros_like(crow_in[:, side])
            grow_in[:, :, side] = jnp.zeros_like(grow_in[:, :, side])
    for side, cond in enumerate((has_prev_x, has_next_x)):
        @pl.when(jnp.logical_not(cond))
        def _(side=side):
            col_in[:, side] = jnp.zeros_like(col_in[:, side])
            gcol_in[:, :, side] = jnp.zeros_like(gcol_in[:, :, side])
    for cond, ref in ((has_below, below), (has_above, above)):
        @pl.when(jnp.logical_not(cond))
        def _(ref=ref):
            ref[...] = jnp.zeros_like(ref)
    for j in range(nz):
        @pl.when(gz > j)
        def _(j=j):
            gather[:, 1, j] = jnp.zeros_like(gather[:, 1, j])

    row_out[:, :, layers * comps :] = jnp.zeros_like(row_out[:, :, layers * comps :])
    crow_out[:, :, half * comps :] = jnp.zeros_like(crow_out[:, :, half * comps :])
    grow_out[...] = jnp.zeros_like(grow_out)

    corner_id = lax.broadcasted_iota(jnp.int32, (rows, 128), 1)
    basis_lane = lax.broadcasted_iota(jnp.int32, (8, 128), 1)
    basis = [(basis_lane == c).astype(jnp.float32) for c in three]
    for level, count in ((0, layers), (1, half)):
        ups = []
        carry = basis
        for layer in range(count):
            carry = times(block(fac, level, layer, 1), carry)
            ups.append(carry)
        turned, back = None, basis
        for layer in reversed(range(count)):
            mat = block(fac, level, layer, 2)
            turned = ups[layer] if turned is None else [
                a + b for a, b in zip(ups[layer], times(mat, turned))
            ]
            back = times(mat, back)
            if layer == count - 1:
                edge = back
        for kind, value in enumerate((ups[-1], turned, back, edge)):
            for c in three:
                maps[gz, level, kind, c] = value[c]

    def held(level, owner, kind, width):
        tiles = [maps[owner, level, kind, c] for c in three]
        return [[jnp.broadcast_to(tiles[i][:rows, j : j + 1], (rows, width)) for j in three] for i in three]

    def send_sides(phase, level, field, count, tail=None):
        out, into = (crow_out, crow_in) if level else (row_out, row_in)
        slot = phase - SWEEPS - 1 if level else phase
        tiles = [jnp.zeros((rows, wide), jnp.float32)] * 2
        for layer in range(count + (tail is not None)):
            for c in three:
                spot = layer * comps + c
                value = field[layer, c] if layer < count else tail[c]
                out[slot, 0, spot : spot + 1, :] = value[rows - 1 : rows, :]
                out[slot, 1, spot : spot + 1, :] = value[0:1, :]
                here = col_id == spot
                tiles[0] = jnp.where(here, value[:, lanes - 1 : lanes], tiles[0])
                tiles[1] = jnp.where(here, value[:, 0:1], tiles[1])
        for side in range(2):
            col_out[phase, side] = tiles[side]
        for side, cond, target in (
            (0, has_next_y, at(gz, gy + 1, gx)), (1, has_prev_y, at(gz, gy - 1, gx)),
        ):
            copy_if(cond, out.at[slot, side], into.at[slot, side],
                    row_ss.at[phase, side], row_rs.at[phase, side], target)
        for side, cond, target in (
            (0, has_next_x, at(gz, gy, gx + 1)), (1, has_prev_x, at(gz, gy, gx - 1)),
        ):
            copy_if(cond, col_out.at[phase, side], col_in.at[phase, side],
                    col_ss.at[phase, side], col_rs.at[phase, side], target)
        return phase, slot, into

    def await_sides(handle):
        phase, slot, into = handle
        for side, cond in enumerate((has_prev_y, has_next_y)):
            arrive_if(cond, into.at[slot, side], row_ss.at[phase, side], row_rs.at[phase, side])
        for side, cond in enumerate((has_prev_x, has_next_x)):
            arrive_if(cond, col_in.at[phase, side], col_ss.at[phase, side], col_rs.at[phase, side])

    def inner_residual(level, field, source, low, high, count):
        for layer in range(count):
            here = [field[layer, c] for c in three]
            side, vert = [], []
            for c in three:
                x = here[c]
                side.append(
                    (jnp.where(first, 0.0, pltpu.roll(x, 1, 1)) + jnp.where(last, 0.0, pltpu.roll(x, lanes - 1, 1)))
                    + (jnp.where(top, 0.0, pltpu.roll(x, 1, 0)) + jnp.where(bottom, 0.0, pltpu.roll(x, rows - 1, 0)))
                )
                under = field[layer - 1, c] if layer else low[c]
                over = field[layer + 1, c] if layer < count - 1 else high[c]
                vert.append(under + over)
            a = times(block(sten, level, layer, 0), here)
            b = times(block(sten, level, layer, 1), side)
            d = times(block(sten, level, layer, 2), vert)
            for c in three:
                res[layer, c] = source[layer, c] - (a[c] - b[c] - d[c])

    rim_row = jnp.logical_or(top, bottom)
    rim_lane = jnp.logical_or(first, last)

    def full_residual(level, layer):
        rim = chal if level else hal
        edge = [
            jnp.where(rim_row, rim[layer, c][:, :lanes], 0.0) + jnp.where(rim_lane, rim[layer, c][:, lanes:], 0.0)
            for c in three
        ]
        extra = times(block(sten, level, layer, 1), edge)
        return [res[layer, c] + extra[c] for c in three]

    def rim_tile(prev_row, next_row, prev_col, next_col):
        return jnp.concatenate(
            [jnp.where(top, prev_row, next_row), jnp.where(first, prev_col, next_col)], axis=1
        )

    def sides_tile(handle, spot):
        phase, slot, into = handle
        return rim_tile(
            into[slot, 0, spot : spot + 1, :], into[slot, 1, spot : spot + 1, :],
            col_in[phase, 0][:, spot : spot + 1], col_in[phase, 1][:, spot : spot + 1],
        )

    def entry(turn, kind, k, c):
        rim = rim_tile(
            grow_in[turn, kind, 0, k, c : c + 1, :], grow_in[turn, kind, 1, k, c : c + 1, :],
            gcol_in[turn, kind, 0, k][:, c : c + 1], gcol_in[turn, kind, 1, k][:, c : c + 1],
        )
        return gather[turn, kind, k, c], rim

    def send_corners(turn, kind, value, wanted):
        for side, line in ((0, rows - 1), (1, 0)):
            for c in three:
                grow_out[turn, kind, side, c : c + 1, :] = value[c][line : line + 1, :]
        for side, lane in ((0, lanes - 1), (1, 0)):
            tile = jnp.zeros((rows, 128), jnp.float32)
            for c in three:
                tile = jnp.where(corner_id == c, value[c][:, lane : lane + 1], tile)
            gcol_out[turn, kind, side] = tile
        for j in range(nz):
            for side in range(2):
                cond, spot = sides_y[side]
                copy_if(jnp.logical_and(wanted(j), cond), grow_out.at[turn, kind, side],
                        grow_in.at[turn, kind, side, gz],
                        gr_ss.at[turn, kind, side, j], gr_rs.at[turn, kind, side, gz], at(j, spot, gx))
                cond, spot = sides_x[side]
                copy_if(jnp.logical_and(wanted(j), cond), gcol_out.at[turn, kind, side],
                        gcol_in.at[turn, kind, side, gz],
                        gc_ss.at[turn, kind, side, j], gc_rs.at[turn, kind, side, gz], at(j, gy, spot))

    def await_corners(turn, kind, j, wanted):
        for side, (there_y, there_x) in enumerate(((has_prev_y, has_prev_x), (has_next_y, has_next_x))):
            arrive_if(jnp.logical_and(wanted, there_y), grow_in.at[turn, kind, side, j],
                      gr_ss.at[turn, kind, side, j], gr_rs.at[turn, kind, side, j])
            arrive_if(jnp.logical_and(wanted, there_x), gcol_in.at[turn, kind, side, j],
                      gc_ss.at[turn, kind, side, j], gc_rs.at[turn, kind, side, j])

    def line_solve(level, turn, resid, count):
        carry = None
        for layer in range(count):
            now = times(block(fac, level, layer, 0), resid(layer))
            if carry is not None:
                now = [a + b for a, b in zip(now, times(block(fac, level, layer, 1), carry))]
            for c in three:
                chain[layer, c] = now[c]
            carry = now
        for c in three:
            gather[turn, 0, gz, c] = carry[c]
        ending = carry
        if nz > 1:
            send_corners(turn, 0, carry, lambda j: jnp.logical_and(gz != j, gz < nz - 1))
            for j in range(nz):
                copy_if(jnp.logical_and(gz != j, gz < nz - 1), gather.at[turn, 0, gz], gather.at[turn, 0, gz],
                        z_ss.at[turn, 0, j], z_rs.at[turn, 0, gz], at(j, gy, gx))
        back = None
        for layer in reversed(range(count)):
            now = [chain[layer, c] for c in three]
            if back is not None:
                now = [a + b for a, b in zip(now, times(block(fac, level, layer, 2), back))]
            for c in three:
                loc[layer, c] = now[c]
            back = now
        for c in three:
            gather[turn, 1, gz, c] = back[c]
        if nz > 1:
            send_corners(turn, 1, back, lambda j: gz > j)
        for j in range(nz):
            copy_if(gz > j, gather.at[turn, 1, gz], gather.at[turn, 1, gz],
                    z_ss.at[turn, 1, j], z_rs.at[turn, 1, gz], at(j, gy, gx))
        handle = send_sides(turn + 1, level, loc, count, ending)
        for j in range(nz - 1):
            arrive_if(gz != j, gather.at[turn, 0, j], z_ss.at[turn, 0, j], z_rs.at[turn, 0, j])
            await_corners(turn, 0, j, gz != j)
        for j in range(1, nz):
            arrive_if(gz < j, gather.at[turn, 1, j], z_ss.at[turn, 1, j], z_rs.at[turn, 1, j])
            await_corners(turn, 1, j, gz < j)
        await_sides(handle)
        full = 3 * lanes
        zero = [jnp.zeros((rows, full), jnp.float32)] * 3
        ins, outs = [zero], [zero]
        for k in range(nz - 1):
            value = []
            for c in three:
                own, rim = entry(turn, 0, k, c)
                rim = jnp.where(gz == k, sides_tile(handle, count * comps + c), rim)
                value.append(jnp.concatenate([own, rim], axis=1))
            if k:
                value = [a + b for a, b in zip(value, times(held(level, k, 0, full), ins[k]))]
            ins.append(value)
        for k in reversed(range(1, nz)):
            value = [jnp.concatenate(entry(turn, 1, k, c), axis=1) for c in three]
            value = [a + b for a, b in zip(value, times(held(level, k, 1, full), ins[k]))]
            if k < nz - 1:
                value = [a + b for a, b in zip(value, times(held(level, k, 2, full), outs[0]))]
            outs.insert(0, value)
        enter, leave = ins[0], outs[0]
        for k in range(1, nz):
            enter = [jnp.where(gz == k, a, b) for a, b in zip(ins[k], enter)]
            leave = [jnp.where(gz == k, a, b) for a, b in zip(outs[k], leave)]
        carry = enter
        for layer in range(count):
            carry = times(block(fac, level, layer, 1), carry)
            for c in three:
                chainx[layer, c] = carry[c]
        rim, fresh = (chal, turn == SWEEPS) if level else (hal, False)
        carry = leave
        for layer in reversed(range(count)):
            carry = [chainx[layer, c] + b for c, b in enumerate(times(block(fac, level, layer, 2), carry))]
            for c in three:
                loc[layer, c] = loc[layer, c] + carry[c][:, :lanes]
                step = sides_tile(handle, layer * comps + c) + carry[c][:, lanes:]
                rim[layer, c] = step if fresh else rim[layer, c] + step
        under = times(held(level, jnp.maximum(gz - 1, 0), 3, lanes), [loc[0, c] for c in three])
        under = [jnp.where(has_below, enter[c][:, :lanes] + under[c], 0.0) for c in three]
        return under, [leave[c][:, :lanes] for c in three]

    pl.semaphore_wait(barrier, total([cond.astype(jnp.int32) for cond, _ in peers]))

    handle = send_sides(0, 0, start, layers)
    copy_if(has_above, start.at[layers - 1], below, zh_ss.at[0], zh_rs.at[0], at(gz + 1, gy, gx))
    copy_if(has_below, start.at[0], above, zh_ss.at[1], zh_rs.at[1], at(gz - 1, gy, gx))
    for j in range(nz):
        copy_if(gz != j, maps.at[gz], maps.at[gz], map_ss.at[j], map_rs.at[gz], at(j, gy, gx))
    arrive_if(has_below, below, zh_ss.at[0], zh_rs.at[0])
    arrive_if(has_above, above, zh_ss.at[1], zh_rs.at[1])
    for sweep in range(SWEEPS + 1):
        field = out_u if sweep else start
        inner_residual(0, field, load, below, above, layers)
        if sweep == SWEEPS:
            break
        if sweep == 0:
            await_sides(handle)
            for layer in range(layers):
                for c in three:
                    hal[layer, c] = sides_tile(handle, layer * comps + c)
            for j in range(nz):
                arrive_if(gz != j, maps.at[j], map_ss.at[j], map_rs.at[j])
        under, over = line_solve(0, sweep, functools.partial(full_residual, 0), layers)
        for layer in range(layers):
            for c in three:
                out_u[layer, c] = field[layer, c] + loc[layer, c]
        for c in three:
            below[c] = below[c] + under[c]
            above[c] = above[c] + over[c]

    for k in range(half):
        pair = [full_residual(0, 2 * k + step) for step in range(2)]
        for c in three:
            crhs[k, c] = pair[0][c] + pair[1][c]
    for sweep in range(SWEEPS):
        if sweep:
            inner_residual(1, cor, crhs, cbelow, cabove, half)
            source = functools.partial(full_residual, 1)
        else:
            def source(layer):
                return [crhs[layer, c] for c in three]
        under, over = line_solve(1, SWEEPS + sweep, source, half)
        for layer in range(half):
            for c in three:
                value = loc[layer, c]
                cor[layer, c] = cor[layer, c] + value if sweep else value
        for c in three:
            cbelow[c] = cbelow[c] + under[c] if sweep else under[c]
            cabove[c] = cabove[c] + over[c] if sweep else over[c]
    for layer in range(layers):
        for c in three:
            out_u[layer, c] = out_u[layer, c] + cor[layer // 2, c]
            hal[layer, c] = hal[layer, c] + chal[layer // 2, c]
    for c in three:
        below[c] = below[c] + cbelow[c]
        above[c] = above[c] + cabove[c]
    inner_residual(0, out_u, load, below, above, layers)
    for layer in range(layers):
        value = full_residual(0, layer)
        for c in three:
            out_r[layer, c] = value[c]
    for cond, copy in pending:
        @pl.when(cond)
        def _(copy=copy):
            copy.wait_send()


def solution(mesh):
    sizes = tuple(mesh.shape[name] for name in ("gz", "gy", "gx"))
    nz = sizes[0]

    def on_device(right_side, start_field, layer_material, stiffness, line_factors):
        layers, comps, rows, lanes = right_side.shape
        half = layers // 2
        wide = -(-(layers + 1) * comps // 128) * 128
        tall, ctall = (-(-(n + 1) * comps // 8) * 8 for n in (layers, half))
        phases = 2 * SWEEPS + 1
        f32 = jnp.float32
        vmem = pl.BlockSpec(memory_space=pltpu.VMEM)
        smem = pl.BlockSpec(memory_space=pltpu.SMEM)
        dma = pltpu.SemaphoreType.DMA
        scratch = [
            pltpu.VMEM((half, comps, rows, lanes), f32),
            pltpu.VMEM((half, comps, rows, lanes), f32),
            pltpu.VMEM((layers, comps, rows, lanes), f32),
            pltpu.VMEM((layers, comps, rows, lanes), f32),
            pltpu.VMEM((layers, comps, rows, lanes), f32),
            pltpu.VMEM((layers, comps, rows, 3 * lanes), f32),
            pltpu.VMEM((layers, comps, rows, 2 * lanes), f32),
            pltpu.VMEM((half, comps, rows, 2 * lanes), f32),
        ]
        scratch += [pltpu.VMEM((comps, rows, lanes), f32)] * 4
        scratch += [pltpu.VMEM((SWEEPS + 1, 2, tall, lanes), f32)] * 2
        scratch += [pltpu.VMEM((SWEEPS, 2, ctall, lanes), f32)] * 2
        scratch += [pltpu.VMEM((phases, 2, rows, wide), f32)] * 2
        scratch += [
            pltpu.VMEM((2 * SWEEPS, 2, nz, comps, rows, lanes), f32),
            pltpu.VMEM((nz, 2, 4, comps, 8, 128), f32),
            pltpu.VMEM((2 * SWEEPS, 2, 2, 8, lanes), f32),
            pltpu.VMEM((2 * SWEEPS, 2, 2, nz, 8, lanes), f32),
            pltpu.VMEM((2 * SWEEPS, 2, 2, rows, 128), f32),
            pltpu.VMEM((2 * SWEEPS, 2, 2, nz, rows, 128), f32),
        ]
        scratch += [dma((phases, 2))] * 4 + [dma((2 * SWEEPS, 2, nz))] * 2
        scratch += [dma((nz,))] * 2 + [dma((2,))] * 2
        scratch += [dma((2 * SWEEPS, 2, 2, nz))] * 4
        out = jax.ShapeDtypeStruct(right_side.shape, f32)
        return pl.pallas_call(
            functools.partial(kernel, sizes),
            out_shape=(out, out),
            in_specs=[smem, smem, smem, vmem, vmem],
            out_specs=(vmem, vmem),
            scratch_shapes=scratch,
            compiler_params=pltpu.CompilerParams(collective_id=0, has_side_effects=True),
        )(layer_material, stiffness.transpose(1, 2, 3, 0), line_factors.transpose(1, 2, 3, 0), right_side, start_field)

    return jax.shard_map(
        on_device,
        mesh=mesh,
        in_specs=(P("gz", None, "gy", "gx"), P("gz", None, "gy", "gx"), P("gz"), P(), P()),
        out_specs=(P("gz", None, "gy", "gx"), P("gz", None, "gy", "gx")),
        check_vma=False,
    )
```

```python
import functools

import jax
import jax.numpy as jnp
from jax import lax
from jax.experimental import pallas as pl
from jax.experimental.pallas import tpu as pltpu
from jax.sharding import PartitionSpec as P

SWEEPS = 3
MESH = pl.DeviceIdType.MESH


def total(terms):
    result = terms[0]
    for term in terms[1:]:
        result = result + term
    return result


def kernel(
    sizes, material, sten, fac, load, start, out_u, out_r,
    cor, crhs, res, loc, chain, chainx, hal, chal, below, above, cbelow, cabove,
    row_out, row_in, crow_out, crow_in, col_out, col_in,
    gather, maps, grow_out, grow_in, gcol_out, gcol_in,
    row_ss, row_rs, col_ss, col_rs, z_ss, z_rs, map_ss, map_rs, zh_ss, zh_rs,
    gr_ss, gr_rs, gc_ss, gc_rs,
):
    nz, ny, nx = sizes
    layers, comps, rows, lanes = load.shape
    half = layers // 2
    gz, gy, gx = (lax.axis_index(name) for name in ("gz", "gy", "gx"))
    wide = col_in.shape[-1]
    row_id = lax.broadcasted_iota(jnp.int32, (rows, lanes), 0)
    lane_id = lax.broadcasted_iota(jnp.int32, (rows, lanes), 1)
    col_id = lax.broadcasted_iota(jnp.int32, (rows, wide), 1)
    top, bottom = row_id == 0, row_id == rows - 1
    first, last = lane_id == 0, lane_id == lanes - 1
    three = range(comps)
    pending = []

    def block(table, level, layer, which):
        mat_id = material[layer * (2 if level else 1)]
        scale = 0.25 if level and table is sten and which == 2 else None
        values = [[table[which, i, j, mat_id] for j in three] for i in three]
        if scale is not None:
            values = [[scale * v for v in line] for line in values]
        return values

    def times(mat, vec):
        return [total([mat[i][j] * vec[j] for j in three]) for i in three]

    def at(z, y, x):
        return {"gz": z, "gy": y, "gx": x}

    def copy_if(cond, src, dst, ss, rs, target):
        copy = pltpu.make_async_remote_copy(
            src_ref=src, dst_ref=dst, send_sem=ss, recv_sem=rs,
            device_id=target, device_id_type=MESH,
        )

        @pl.when(cond)
        def _():
            copy.start()

        pending.append((cond, copy))

    def arrive_if(cond, ref, ss, rs):
        @pl.when(cond)
        def _():
            pltpu.make_async_remote_copy(
                src_ref=ref, dst_ref=ref, send_sem=ss, recv_sem=rs,
                device_id=at(gz, gy, gx), device_id_type=MESH,
            ).wait_recv()

    has_prev_y, has_next_y = gy > 0, gy < ny - 1
    has_prev_x, has_next_x = gx > 0, gx < nx - 1
    has_below, has_above = gz > 0, gz < nz - 1

    barrier = pltpu.get_barrier_semaphore()
    peers = [(gz != j, at(j, gy, gx)) for j in range(nz)]
    peers += [(has_prev_y, at(gz, gy - 1, gx)), (has_next_y, at(gz, gy + 1, gx))]
    peers += [(has_prev_x, at(gz, gy, gx - 1)), (has_next_x, at(gz, gy, gx + 1))]
    sides_y = ((has_next_y, gy + 1), (has_prev_y, gy - 1))
    sides_x = ((has_next_x, gx + 1), (has_prev_x, gx - 1))
    for j in range(nz):
        peers += [(jnp.logical_and(gz != j, cond), at(j, spot, gx)) for cond, spot in sides_y]
        peers += [(jnp.logical_and(gz != j, cond), at(j, gy, spot)) for cond, spot in sides_x]
    for cond, target in peers:
        @pl.when(cond)
        def _(target=target):
            pl.semaphore_signal(barrier, inc=1, device_id=target, device_id_type=MESH)

    for side, cond in enumerate((has_prev_y, has_next_y)):
        @pl.when(jnp.logical_not(cond))
        def _(side=side):
            row_in[:, side] = jnp.zeros_like(row_in[:, side])
            crow_in[:, side] = jnp.zeros_like(crow_in[:, side])
            grow_in[:, :, side] = jnp.zeros_like(grow_in[:, :, side])
    for side, cond in enumerate((has_prev_x, has_next_x)):
        @pl.when(jnp.logical_not(cond))
        def _(side=side):
            col_in[:, side] = jnp.zeros_like(col_in[:, side])
            gcol_in[:, :, side] = jnp.zeros_like(gcol_in[:, :, side])
    for cond, ref in ((has_below, below), (has_above, above)):
        @pl.when(jnp.logical_not(cond))
        def _(ref=ref):
            ref[...] = jnp.zeros_like(ref)
    for j in range(nz):
        @pl.when(gz > j)
        def _(j=j):
            gather[:, 1, j] = jnp.zeros_like(gather[:, 1, j])

    row_out[:, :, layers * comps :] = jnp.zeros_like(row_out[:, :, layers * comps :])
    crow_out[:, :, half * comps :] = jnp.zeros_like(crow_out[:, :, half * comps :])
    grow_out[...] = jnp.zeros_like(grow_out)

    corner_id = lax.broadcasted_iota(jnp.int32, (rows, 128), 1)
    basis_lane = lax.broadcasted_iota(jnp.int32, (8, 128), 1)
    basis = [(basis_lane == c).astype(jnp.float32) for c in three]
    for level, count in ((0, layers), (1, half)):
        ups = []
        carry = basis
        for layer in range(count):
            carry = times(block(fac, level, layer, 1), carry)
            ups.append(carry)
        turned, back = None, basis
        for layer in reversed(range(count)):
            mat = block(fac, level, layer, 2)
            turned = ups[layer] if turned is None else [
                a + b for a, b in zip(ups[layer], times(mat, turned))
            ]
            back = times(mat, back)
            if layer == count - 1:
                edge = back
        for kind, value in enumerate((ups[-1], turned, back, edge)):
            for c in three:
                maps[gz, level, kind, c] = value[c]

    def held(level, owner, kind, width):
        tiles = [maps[owner, level, kind, c] for c in three]
        return [[jnp.broadcast_to(tiles[i][:rows, j : j + 1], (rows, width)) for j in three] for i in three]

    def send_sides(phase, level, field, count, tail=None):
        out, into = (crow_out, crow_in) if level else (row_out, row_in)
        slot = phase - SWEEPS - 1 if level else phase
        tiles = [jnp.zeros((rows, wide), jnp.float32)] * 2
        for layer in range(count + (tail is not None)):
            for c in three:
                spot = layer * comps + c
                value = field[layer, c] if layer < count else tail[c]
                out[slot, 0, spot : spot + 1, :] = value[rows - 1 : rows, :]
                out[slot, 1, spot : spot + 1, :] = value[0:1, :]
                here = col_id == spot
                tiles[0] = jnp.where(here, value[:, lanes - 1 : lanes], tiles[0])
                tiles[1] = jnp.where(here, value[:, 0:1], tiles[1])
        for side in range(2):
            col_out[phase, side] = tiles[side]
        for side, cond, target in (
            (0, has_next_y, at(gz, gy + 1, gx)), (1, has_prev_y, at(gz, gy - 1, gx)),
        ):
            copy_if(cond, out.at[slot, side], into.at[slot, side],
                    row_ss.at[phase, side], row_rs.at[phase, side], target)
        for side, cond, target in (
            (0, has_next_x, at(gz, gy, gx + 1)), (1, has_prev_x, at(gz, gy, gx - 1)),
        ):
            copy_if(cond, col_out.at[phase, side], col_in.at[phase, side],
                    col_ss.at[phase, side], col_rs.at[phase, side], target)
        return phase, slot, into

    def await_sides(handle):
        phase, slot, into = handle
        for side, cond in enumerate((has_prev_y, has_next_y)):
            arrive_if(cond, into.at[slot, side], row_ss.at[phase, side], row_rs.at[phase, side])
        for side, cond in enumerate((has_prev_x, has_next_x)):
            arrive_if(cond, col_in.at[phase, side], col_ss.at[phase, side], col_rs.at[phase, side])

    def inner_residual(level, field, source, low, high, count):
        for layer in range(count):
            here = [field[layer, c] for c in three]
            side, vert = [], []
            for c in three:
                x = here[c]
                side.append(
                    (jnp.where(first, 0.0, pltpu.roll(x, 1, 1)) + jnp.where(last, 0.0, pltpu.roll(x, lanes - 1, 1)))
                    + (jnp.where(top, 0.0, pltpu.roll(x, 1, 0)) + jnp.where(bottom, 0.0, pltpu.roll(x, rows - 1, 0)))
                )
                under = field[layer - 1, c] if layer else low[c]
                over = field[layer + 1, c] if layer < count - 1 else high[c]
                vert.append(under + over)
            a = times(block(sten, level, layer, 0), here)
            b = times(block(sten, level, layer, 1), side)
            d = times(block(sten, level, layer, 2), vert)
            for c in three:
                res[layer, c] = source[layer, c] - (a[c] - b[c] - d[c])

    rim_row = jnp.logical_or(top, bottom)
    rim_lane = jnp.logical_or(first, last)

    def full_residual(level, layer):
        rim = chal if level else hal
        edge = [
            jnp.where(rim_row, rim[layer, c][:, :lanes], 0.0) + jnp.where(rim_lane, rim[layer, c][:, lanes:], 0.0)
            for c in three
        ]
        extra = times(block(sten, level, layer, 1), edge)
        return [res[layer, c] + extra[c] for c in three]

    def rim_tile(prev_row, next_row, prev_col, next_col):
        return jnp.concatenate(
            [jnp.where(top, prev_row, next_row), jnp.where(first, prev_col, next_col)], axis=1
        )

    def sides_tile(handle, spot):
        phase, slot, into = handle
        return rim_tile(
            into[slot, 0, spot : spot + 1, :], into[slot, 1, spot : spot + 1, :],
            col_in[phase, 0][:, spot : spot + 1], col_in[phase, 1][:, spot : spot + 1],
        )

    def entry(turn, kind, k, c):
        rim = rim_tile(
            grow_in[turn, kind, 0, k, c : c + 1, :], grow_in[turn, kind, 1, k, c : c + 1, :],
            gcol_in[turn, kind, 0, k][:, c : c + 1], gcol_in[turn, kind, 1, k][:, c : c + 1],
        )
        return gather[turn, kind, k, c], rim

    def send_corners(turn, kind, value, wanted):
        for side, line in ((0, rows - 1), (1, 0)):
            for c in three:
                grow_out[turn, kind, side, c : c + 1, :] = value[c][line : line + 1, :]
        for side, lane in ((0, lanes - 1), (1, 0)):
            tile = jnp.zeros((rows, 128), jnp.float32)
            for c in three:
                tile = jnp.where(corner_id == c, value[c][:, lane : lane + 1], tile)
            gcol_out[turn, kind, side] = tile
        for j in range(nz):
            for side in range(2):
                cond, spot = sides_y[side]
                copy_if(jnp.logical_and(wanted(j), cond), grow_out.at[turn, kind, side],
                        grow_in.at[turn, kind, side, gz],
                        gr_ss.at[turn, kind, side, j], gr_rs.at[turn, kind, side, gz], at(j, spot, gx))
                cond, spot = sides_x[side]
                copy_if(jnp.logical_and(wanted(j), cond), gcol_out.at[turn, kind, side],
                        gcol_in.at[turn, kind, side, gz],
                        gc_ss.at[turn, kind, side, j], gc_rs.at[turn, kind, side, gz], at(j, gy, spot))

    def await_corners(turn, kind, j, wanted):
        for side, (there_y, there_x) in enumerate(((has_prev_y, has_prev_x), (has_next_y, has_next_x))):
            arrive_if(jnp.logical_and(wanted, there_y), grow_in.at[turn, kind, side, j],
                      gr_ss.at[turn, kind, side, j], gr_rs.at[turn, kind, side, j])
            arrive_if(jnp.logical_and(wanted, there_x), gcol_in.at[turn, kind, side, j],
                      gc_ss.at[turn, kind, side, j], gc_rs.at[turn, kind, side, j])

    def line_solve(level, turn, resid, count):
        carry = None
        for layer in range(count):
            now = times(block(fac, level, layer, 0), resid(layer))
            if carry is not None:
                now = [a + b for a, b in zip(now, times(block(fac, level, layer, 1), carry))]
            for c in three:
                chain[layer, c] = now[c]
            carry = now
        for c in three:
            gather[turn, 0, gz, c] = carry[c]
        ending = carry
        if nz > 1:
            send_corners(turn, 0, carry, lambda j: jnp.logical_and(gz != j, gz < nz - 1))
            for j in range(nz):
                copy_if(jnp.logical_and(gz != j, gz < nz - 1), gather.at[turn, 0, gz], gather.at[turn, 0, gz],
                        z_ss.at[turn, 0, j], z_rs.at[turn, 0, gz], at(j, gy, gx))
        back = None
        for layer in reversed(range(count)):
            now = [chain[layer, c] for c in three]
            if back is not None:
                now = [a + b for a, b in zip(now, times(block(fac, level, layer, 2), back))]
            for c in three:
                loc[layer, c] = now[c]
            back = now
        for c in three:
            gather[turn, 1, gz, c] = back[c]
        if nz > 1:
            send_corners(turn, 1, back, lambda j: gz > j)
        for j in range(nz):
            copy_if(gz > j, gather.at[turn, 1, gz], gather.at[turn, 1, gz],
                    z_ss.at[turn, 1, j], z_rs.at[turn, 1, gz], at(j, gy, gx))
        handle = send_sides(turn + 1, level, loc, count, ending)
        await_sides(handle)
        halo, fresh = (chal, turn == SWEEPS) if level else (hal, False)
        for layer in range(count):
            for c in three:
                step = sides_tile(handle, layer * comps + c)
                halo[layer, c] = step if fresh else halo[layer, c] + step
        for j in range(nz - 1):
            arrive_if(gz != j, gather.at[turn, 0, j], z_ss.at[turn, 0, j], z_rs.at[turn, 0, j])
            await_corners(turn, 0, j, gz != j)
        for j in range(1, nz):
            arrive_if(gz < j, gather.at[turn, 1, j], z_ss.at[turn, 1, j], z_rs.at[turn, 1, j])
            await_corners(turn, 1, j, gz < j)
        full = 3 * lanes
        zero = [jnp.zeros((rows, full), jnp.float32)] * 3
        ins, outs = [zero], [zero]
        for k in range(nz - 1):
            value = []
            for c in three:
                own, rim = entry(turn, 0, k, c)
                rim = jnp.where(gz == k, sides_tile(handle, count * comps + c), rim)
                value.append(jnp.concatenate([own, rim], axis=1))
            if k:
                value = [a + b for a, b in zip(value, times(held(level, k, 0, full), ins[k]))]
            ins.append(value)
        for k in reversed(range(1, nz)):
            value = [jnp.concatenate(entry(turn, 1, k, c), axis=1) for c in three]
            value = [a + b for a, b in zip(value, times(held(level, k, 1, full), ins[k]))]
            if k < nz - 1:
                value = [a + b for a, b in zip(value, times(held(level, k, 2, full), outs[0]))]
            outs.insert(0, value)
        enter, leave = ins[0], outs[0]
        for k in range(1, nz):
            enter = [jnp.where(gz == k, a, b) for a, b in zip(ins[k], enter)]
            leave = [jnp.where(gz == k, a, b) for a, b in zip(outs[k], leave)]
        carry = enter
        for layer in range(count):
            carry = times(block(fac, level, layer, 1), carry)
            for c in three:
                chainx[layer, c] = carry[c]
        carry = leave
        for layer in reversed(range(count)):
            carry = [chainx[layer, c] + b for c, b in enumerate(times(block(fac, level, layer, 2), carry))]
            for c in three:
                loc[layer, c] = loc[layer, c] + carry[c][:, :lanes]
                halo[layer, c] = halo[layer, c] + carry[c][:, lanes:]
        under = times(held(level, jnp.maximum(gz - 1, 0), 3, lanes), [loc[0, c] for c in three])
        under = [jnp.where(has_below, enter[c][:, :lanes] + under[c], 0.0) for c in three]
        return under, [leave[c][:, :lanes] for c in three]

    pl.semaphore_wait(barrier, total([cond.astype(jnp.int32) for cond, _ in peers]))

    handle = send_sides(0, 0, start, layers)
    copy_if(has_above, start.at[layers - 1], below, zh_ss.at[0], zh_rs.at[0], at(gz + 1, gy, gx))
    copy_if(has_below, start.at[0], above, zh_ss.at[1], zh_rs.at[1], at(gz - 1, gy, gx))
    for j in range(nz):
        copy_if(gz != j, maps.at[gz], maps.at[gz], map_ss.at[j], map_rs.at[gz], at(j, gy, gx))
    arrive_if(has_below, below, zh_ss.at[0], zh_rs.at[0])
    arrive_if(has_above, above, zh_ss.at[1], zh_rs.at[1])
    for sweep in range(SWEEPS + 1):
        field = out_u if sweep else start
        inner_residual(0, field, load, below, above, layers)
        if sweep == SWEEPS:
            break
        if sweep == 0:
            await_sides(handle)
            for layer in range(layers):
                for c in three:
                    hal[layer, c] = sides_tile(handle, layer * comps + c)
            for j in range(nz):
                arrive_if(gz != j, maps.at[j], map_ss.at[j], map_rs.at[j])
        under, over = line_solve(0, sweep, functools.partial(full_residual, 0), layers)
        for layer in range(layers):
            for c in three:
                out_u[layer, c] = field[layer, c] + loc[layer, c]
        for c in three:
            below[c] = below[c] + under[c]
            above[c] = above[c] + over[c]

    for k in range(half):
        pair = [full_residual(0, 2 * k + step) for step in range(2)]
        for c in three:
            crhs[k, c] = pair[0][c] + pair[1][c]
    for sweep in range(SWEEPS):
        if sweep:
            inner_residual(1, cor, crhs, cbelow, cabove, half)
            source = functools.partial(full_residual, 1)
        else:
            def source(layer):
                return [crhs[layer, c] for c in three]
        under, over = line_solve(1, SWEEPS + sweep, source, half)
        for layer in range(half):
            for c in three:
                value = loc[layer, c]
                cor[layer, c] = cor[layer, c] + value if sweep else value
        for c in three:
            cbelow[c] = cbelow[c] + under[c] if sweep else under[c]
            cabove[c] = cabove[c] + over[c] if sweep else over[c]
    for layer in range(layers):
        for c in three:
            out_u[layer, c] = out_u[layer, c] + cor[layer // 2, c]
            hal[layer, c] = hal[layer, c] + chal[layer // 2, c]
    for c in three:
        below[c] = below[c] + cbelow[c]
        above[c] = above[c] + cabove[c]
    inner_residual(0, out_u, load, below, above, layers)
    for layer in range(layers):
        value = full_residual(0, layer)
        for c in three:
            out_r[layer, c] = value[c]
    for cond, copy in pending:
        @pl.when(cond)
        def _(copy=copy):
            copy.wait_send()


def solution(mesh):
    sizes = tuple(mesh.shape[name] for name in ("gz", "gy", "gx"))
    nz = sizes[0]

    def on_device(right_side, start_field, layer_material, stiffness, line_factors):
        layers, comps, rows, lanes = right_side.shape
        half = layers // 2
        wide = -(-(layers + 1) * comps // 128) * 128
        tall, ctall = (-(-(n + 1) * comps // 8) * 8 for n in (layers, half))
        phases = 2 * SWEEPS + 1
        f32 = jnp.float32
        vmem = pl.BlockSpec(memory_space=pltpu.VMEM)
        smem = pl.BlockSpec(memory_space=pltpu.SMEM)
        dma = pltpu.SemaphoreType.DMA
        scratch = [
            pltpu.VMEM((half, comps, rows, lanes), f32),
            pltpu.VMEM((half, comps, rows, lanes), f32),
            pltpu.VMEM((layers, comps, rows, lanes), f32),
            pltpu.VMEM((layers, comps, rows, lanes), f32),
            pltpu.VMEM((layers, comps, rows, lanes), f32),
            pltpu.VMEM((layers, comps, rows, 3 * lanes), f32),
            pltpu.VMEM((layers, comps, rows, 2 * lanes), f32),
            pltpu.VMEM((half, comps, rows, 2 * lanes), f32),
        ]
        scratch += [pltpu.VMEM((comps, rows, lanes), f32)] * 4
        scratch += [pltpu.VMEM((SWEEPS + 1, 2, tall, lanes), f32)] * 2
        scratch += [pltpu.VMEM((SWEEPS, 2, ctall, lanes), f32)] * 2
        scratch += [pltpu.VMEM((phases, 2, rows, wide), f32)] * 2
        scratch += [
            pltpu.VMEM((2 * SWEEPS, 2, nz, comps, rows, lanes), f32),
            pltpu.VMEM((nz, 2, 4, comps, 8, 128), f32),
            pltpu.VMEM((2 * SWEEPS, 2, 2, 8, lanes), f32),
            pltpu.VMEM((2 * SWEEPS, 2, 2, nz, 8, lanes), f32),
            pltpu.VMEM((2 * SWEEPS, 2, 2, rows, 128), f32),
            pltpu.VMEM((2 * SWEEPS, 2, 2, nz, rows, 128), f32),
        ]
        scratch += [dma((phases, 2))] * 4 + [dma((2 * SWEEPS, 2, nz))] * 2
        scratch += [dma((nz,))] * 2 + [dma((2,))] * 2
        scratch += [dma((2 * SWEEPS, 2, 2, nz))] * 4
        out = jax.ShapeDtypeStruct(right_side.shape, f32)
        return pl.pallas_call(
            functools.partial(kernel, sizes),
            out_shape=(out, out),
            in_specs=[smem, smem, smem, vmem, vmem],
            out_specs=(vmem, vmem),
            scratch_shapes=scratch,
            compiler_params=pltpu.CompilerParams(collective_id=0, has_side_effects=True),
        )(layer_material, stiffness.transpose(1, 2, 3, 0), line_factors.transpose(1, 2, 3, 0), right_side, start_field)

    return jax.shard_map(
        on_device,
        mesh=mesh,
        in_specs=(P("gz", None, "gy", "gx"), P("gz", None, "gy", "gx"), P("gz"), P(), P()),
        out_specs=(P("gz", None, "gy", "gx"), P("gz", None, "gy", "gx")),
        check_vma=False,
    )
```
